256 devices in a mesh: blk: 128 (over y, x_lo, z, core), rep: 2 (over x_hi).
Axes of the slice: x: 4 (x_hi: 2, x_lo: 2; x = x_hi * 2 + x_lo), y: 4, z: 8, core: 2. Of those that a mesh axis runs over, the one named last changes fastest.
Arguments:
- queries: bfloat16 [32768, 1024], P('blk'), may hold values from -20 to 20
- corpus: bfloat16 [2, 262144, 1024], P('rep', 'blk'), may hold values from -5 to 5
- attributions: bfloat16 [2, 262144, 1024], P('rep', 'blk'), may hold values from -6 to 6
Outputs:
- attributed: bfloat16 [32768, 1024], P('blk')
- log_total: float32 [32768], P('blk')
The draws below stay inside these ranges and needn't reach their ends.
All inputs are finite; a program needn't handle non-finite values.
Results may differ from the reference program's by a relative error of at most 0.003.
Values may be sent and summed in bfloat16 or wider, within the bound.
A program may use at most 64 MiB of HBM per device.

```python
import jax
import jax.numpy as jnp
from jax import lax

D = 1024
DV = 1024
Q_DEV = 256
C_DEV = 2048
STEPS = 4
QUERIES = 32768
SLAB_ROWS = 262144
N_BLK = 128
N_REP = 2


def corpus_base(key):
    return jax.random.truncated_normal(jax.random.fold_in(key, 11), -5.0, 5.0, (N_REP, SLAB_ROWS, D), jnp.float32)


def draw_corpus(key, part):
    base = corpus_base(key)
    return base.astype(jnp.bfloat16)


def draw_queries(key, part):
    noise = jax.random.truncated_normal(jax.random.fold_in(key, 23), -5.0, 5.0, (QUERIES, D), jnp.float32)
    return noise.astype(jnp.bfloat16)


def block_levels(rng, dims, cuts, least, top_value):
    def one(dim, shards_of):
        draws = jax.random.uniform(jax.random.fold_in(jax.random.fold_in(rng, 6), dim), (shards_of,), jnp.float32, least / len(cuts), top_value / len(cuts))
        return jnp.repeat(jnp.exp(draws), dims[dim] // shards_of).reshape((-1,) + (1,) * (len(dims) - dim - 1))

    loudness = one(*cuts[0])
    for cut in cuts[1:]:
        loudness = loudness * one(*cut)
    return loudness


def centred(own_key, extent, scale, reach, cuts=(), held_as=jnp.bfloat16):
    entries = scale * jax.random.normal(own_key, extent, jnp.float32)
    if cuts:
        entries = entries * block_levels(own_key, extent, cuts, -0.22, 0.18)
    return jnp.clip(entries, -reach, reach).astype(held_as)


def setup_inputs(seed: int = 0) -> dict:
    seeds = jax.random.split(jax.random.key(seed), 4)
    queries = draw_queries(jax.random.fold_in(seeds[3], 71), 0)
    corpus = draw_corpus(jax.random.fold_in(seeds[3], 71), 0)
    attributions = centred(seeds[2], (N_REP, SLAB_ROWS, DV), 1.0, 6.0, ((0, 2), (1, 128)))
    return dict(queries=queries, corpus=corpus, attributions=attributions)


sharpness = 2.5

def partial_stats(block_queries, slab_keys, slab_values):
    scores = jnp.dot(block_queries, slab_keys.T, preferred_element_type=jnp.float32) * (sharpness / jnp.sqrt(jnp.float32(block_queries.shape[1])))
    row_max = lax.optimization_barrier(jnp.max(scores, axis=1))
    weights = jnp.exp(scores - row_max[:, None])
    row_sum = lax.optimization_barrier(jnp.sum(weights, axis=1))
    weighted = jnp.dot(weights.astype(jnp.bfloat16), slab_values, preferred_element_type=jnp.float32)
    return (row_max, row_sum, weighted)

def combine(left_part, right_part):
    joined = jnp.maximum(left_part[0], right_part[0])
    left_factor = jnp.exp(left_part[0] - joined)
    right_factor = jnp.exp(right_part[0] - joined)
    row_sum = left_part[1] * left_factor + right_part[1] * right_factor
    weighted = left_part[2] * left_factor[:, None] + right_part[2] * right_factor[:, None]
    return (joined, row_sum, weighted)

def reference(queries, corpus, attributions):
    query_blocks = queries.reshape(N_BLK, Q_DEV, D)
    key_slabs = corpus.reshape(N_REP, N_BLK, C_DEV, D)
    value_slabs = attributions.reshape(N_REP, N_BLK, C_DEV, DV)

    def one_block(block_index):
        block_queries = lax.dynamic_index_in_dim(query_blocks, block_index, 0, keepdims=False)
        running = None
        for quarter in range(N_REP):
            for offset in range(STEPS):
                slab = ((block_index + offset) % N_BLK).astype(jnp.int32)
                slab_keys = lax.dynamic_index_in_dim(key_slabs[quarter], slab, 0, keepdims=False)
                slab_values = lax.dynamic_index_in_dim(value_slabs[quarter], slab, 0, keepdims=False)
                stats = partial_stats(block_queries, slab_keys, slab_values)
                running = stats if running is None else combine(running, stats)
        attributed = (running[2] / running[1][:, None]).astype(jnp.bfloat16)
        log_total = running[0] + jnp.log(running[1])
        return (attributed, log_total)
    attributed, log_total = lax.map(one_block, jnp.arange(N_BLK, dtype=jnp.int32))
    return (attributed.reshape(QUERIES, DV), log_total.reshape(QUERIES))
```

```python
import functools
import math

import jax
import jax.numpy as jnp
from jax import lax
from jax.experimental import pallas as pl
from jax.experimental.pallas import tpu as pltpu
from jax.sharding import PartitionSpec as P

MESH = pl.DeviceIdType.MESH
SHARPNESS = 2.5
PARTS = 2
TO_NEXT_CHIP, TO_NEXT, TO_CORE, SIDE, SIDE_L, BACK, BACK_L, OWN, OWN_L, HOME, HOME_L, HOME2, HOME2_L, FINAL = range(14)
NEVER = -1e30


def as_column(tile, rows):
    return jnp.broadcast_to(tile[0:1], (128, rows)).T[:, 0:1]


def as_tile(column, rows):
    return jnp.broadcast_to(column, (rows, 128)).T[0:8]


def log_sum(terms):
    top = functools.reduce(jnp.maximum, terms)
    return top + jnp.log(sum(jnp.exp(t - top) for t in terms))


def kernel(
    n, q_hbm, k_hbm, v_hbm, out_hbm, log_ref,
    qs, ks, vs, pf, r1, p3, r3, xs, rx, ms, rm, own, fin, lp, l1, l3, lo, lx, lm, lr,
    load_sem, send_sem, recv_sem, out_sem,
):
    b = lax.axis_index("blk")
    r = lax.axis_index("rep")
    c = lax.rem(b, 2)
    block, depth = q_hbm.shape
    half = vs.shape[1] // 2
    rows = block // PARTS

    def at(step, rep=None):
        return (lax.rem(b + n + step, n), r if rep is None else rep)

    partner = at(1 - 2 * c)

    def part(g):
        return pl.ds(g * rows, rows)

    def remote(kind, g, src, dst, device, land=None):
        return pltpu.make_async_remote_copy(
            src_ref=src, dst_ref=dst,
            send_sem=send_sem.at[kind, g],
            recv_sem=recv_sem.at[kind if land is None else land, g],
            device_id=device, device_id_type=MESH,
        )

    loads = [pltpu.make_async_copy(q_hbm, qs.at[0], load_sem.at[0]),
             pltpu.make_async_copy(k_hbm.at[0], ks, load_sem.at[1]),
             pltpu.make_async_copy(v_hbm.at[0], vs, load_sem.at[2])]
    for load in loads:
        load.start()

    barrier = pltpu.get_barrier_semaphore()
    for device in (at(-2), at(-1), at(1), at(2), at(2, 1 - r), at(0, 1 - r)):
        pl.semaphore_signal(barrier, inc=1, device_id=device, device_id_type=MESH)
    pl.semaphore_wait(barrier, 6)

    def next_chip(g):
        return remote(TO_NEXT_CHIP, g, qs.at[0, part(g)], qs.at[2, part(g)], at(2))

    def next_block(g):
        return remote(TO_NEXT, g, qs.at[2, part(g)], qs.at[3, part(g)], at(1))

    def next_core(g):
        return remote(TO_CORE, g, qs.at[2 * c, part(g)], qs.at[1, part(g)], partner)

    def side(g):
        return (remote(SIDE, g, pf.at[1, :, part(g)], r1.at[:, part(g)], partner),
                remote(SIDE_L, g, lp.at[1, g], l1.at[g], partner))

    def back(g):
        return (remote(BACK, g, p3.at[:, part(g)], r3.at[:, part(g)], at(-1)),
                remote(BACK_L, g, lp.at[3, g], l3.at[g], at(-1)))

    def across(g):
        return (remote(OWN, g, xs.at[part(g)], rx.at[part(g)], at(0, 1 - r)),
                remote(OWN_L, g, lo.at[g], lx.at[g], at(0, 1 - r)))

    def home(g, j, source):
        return (remote(HOME + 2 * j, g, ms.at[j, part(g)], rm.at[source, part(g)], at(-2, j), HOME + 2 * source),
                remote(HOME_L + 2 * j, g, lm.at[g], lr.at[source, g], at(-2, j), HOME_L + 2 * source))

    def final(g, column):
        return remote(FINAL, g, fin.at[part(g)], out_hbm.at[part(g), column], at(0, 1 - r))

    def start(*copies):
        for copy in copies:
            copy.start()

    def arrived(*copies):
        for copy in copies:
            copy.wait_recv()

    scale = SHARPNESS / math.sqrt(depth)

    def attend(slot, g):
        d = lax.dot_general(qs[slot, part(g)], ks[...], (((1,), (1,)), ((), ())), preferred_element_type=jnp.float32)
        top = jnp.max(d, axis=1, keepdims=True)
        weights = jnp.exp2((d - top) * (scale * math.log2(math.e)))
        total = jnp.sum(weights, axis=1, keepdims=True)
        low = weights.astype(jnp.bfloat16)
        share = 1.0 / total
        for j in range(2):
            pf[slot, j, part(g)] = share * jnp.dot(low, vs[:, j * half:(j + 1) * half], preferred_element_type=jnp.float32)
        lp[slot, g] = as_tile(top * scale + jnp.log(total), rows)

    loads[0].wait()

    @pl.when(c == 0)
    def _():
        for g in range(PARTS):
            next_core(g).start()

    for g in range(PARTS):
        next_chip(g).start()
    loads[1].wait()
    loads[2].wait()
    for g in range(PARTS):
        attend(0, g)

    for g in range(PARTS):
        @pl.when(c == 1)
        def _():
            arrived(next_chip(g))
            start(next_block(g), next_core(g))
        arrived(next_core(g))
        attend(1, g)
        start(*side(g))

    def returned(g):
        p3[:, part(g)] = pf[3, :, part(g)].astype(jnp.bfloat16)
        start(*back(g))

    for g in range(PARTS):
        @pl.when(c == 0)
        def _():
            arrived(next_chip(g))
            start(next_block(g))
            arrived(next_block(g))
        attend(3 - c, g)

        @pl.when(c == 0)
        def _():
            returned(g)

    for g in range(PARTS):
        arrived(*side(g))
        ours = as_column(lp[0, g], rows)
        theirs = jnp.where(c == 0, as_column(l1[g], rows), NEVER)
        both = log_sum([ours, theirs])
        ours, theirs = jnp.exp(ours - both), jnp.exp(theirs - both)
        xs[part(g)] = (ours * pf[0, 1 - r, part(g)] + theirs * r1[1 - r, part(g)]).astype(jnp.bfloat16)
        own[part(g)] = ours * pf[0, r, part(g)] + theirs * r1[r, part(g)]
        lo[g] = as_tile(both, rows)
        start(*across(g))

    for g in range(PARTS):
        @pl.when(c == 1)
        def _():
            arrived(next_block(g))
        attend(2 + c, g)

        @pl.when(c == 1)
        def _():
            returned(g)
        arrived(*back(g))
        mine = as_column(lp[2, g], rows)
        core = jnp.where(c == 1, as_column(l1[g], rows), NEVER)
        behind = as_column(l3[g], rows)
        both = log_sum([mine, core, behind])
        mine, core, behind = jnp.exp(mine - both), jnp.exp(core - both), jnp.exp(behind - both)
        lm[g] = as_tile(both, rows)
        for j in range(2):
            ms[j, part(g)] = (mine * pf[2, j, part(g)] + core * r1[j, part(g)]
                              + behind * r3[j, part(g)].astype(jnp.float32)).astype(jnp.bfloat16)
            start(*home(g, j, r))

    column = pl.ds(pl.multiple_of(r * half, half), half)
    outs = []
    for g in range(PARTS):
        arrived(*across(g), *home(g, 0, 0), *home(g, 1, 1))
        logs = [as_column(t, rows) for t in (lo[g], lx[g], lr[0, g], lr[1, g])]
        both = log_sum(logs)
        w = [jnp.exp(t - both) for t in logs]
        fin[part(g)] = (w[0] * own[part(g)] + w[1] * rx[part(g)].astype(jnp.float32)
                        + w[2] * rm[0, part(g)].astype(jnp.float32)
                        + w[3] * rm[1, part(g)].astype(jnp.float32)).astype(jnp.bfloat16)
        final(g, column).start()
        out = pltpu.make_async_copy(fin.at[part(g)], out_hbm.at[part(g), column], out_sem.at[g])
        out.start()
        outs.append(out)
        log_ref[g:g + 1] = as_tile(both, rows)[0:1]

    for out in outs:
        out.wait()
    for g in range(PARTS):
        arrived(final(g, column))
        for copy in (next_chip(g), next_block(g), next_core(g), *side(g), *back(g), *across(g),
                     *home(g, 0, r), *home(g, 1, r), final(g, column)):
            copy.wait_send()


def shards(n, queries, corpus, attributions):
    block, depth = queries.shape
    slab, width = attributions.shape[1:]
    rows, half = block // PARTS, width // 2
    low, full = jnp.bfloat16, jnp.float32
    hbm = pl.BlockSpec(memory_space=pl.ANY)
    attributed, log_total = pl.pallas_call(
        functools.partial(kernel, n),
        out_shape=(jax.ShapeDtypeStruct((block, width), low), jax.ShapeDtypeStruct((PARTS, rows), full)),
        in_specs=[hbm] * 3,
        out_specs=(hbm, pl.BlockSpec(memory_space=pltpu.VMEM)),
        scratch_shapes=[
            pltpu.VMEM((4, block, depth), low),
            pltpu.VMEM((slab, depth), low),
            pltpu.VMEM((slab, width), low),
            pltpu.VMEM((4, 2, block, half), full),
            pltpu.VMEM((2, block, half), full),
            pltpu.VMEM((2, block, half), low),
            pltpu.VMEM((2, block, half), low),
            pltpu.VMEM((block, half), low),
            pltpu.VMEM((block, half), low),
            pltpu.VMEM((2, block, half), low),
            pltpu.VMEM((2, block, half), low),
            pltpu.VMEM((block, half), full),
            pltpu.VMEM((block, half), low),
            pltpu.VMEM((4, PARTS, 8, rows), full),
            pltpu.VMEM((PARTS, 8, rows), full),
            pltpu.VMEM((PARTS, 8, rows), full),
            pltpu.VMEM((PARTS, 8, rows), full),
            pltpu.VMEM((PARTS, 8, rows), full),
            pltpu.VMEM((PARTS, 8, rows), full),
            pltpu.VMEM((2, PARTS, 8, rows), full),
            pltpu.SemaphoreType.DMA((3,)),
            pltpu.SemaphoreType.DMA((14, PARTS)),
            pltpu.SemaphoreType.DMA((14, PARTS)),
            pltpu.SemaphoreType.DMA((PARTS,)),
        ],
        compiler_params=pltpu.CompilerParams(collective_id=0, has_side_effects=True, vmem_limit_bytes=60 << 20),
    )(queries, corpus, attributions)
    return attributed, log_total.reshape(block)


def solution(mesh):
    return jax.shard_map(
        functools.partial(shards, mesh.shape["blk"]),
        mesh=mesh,
        in_specs=(P("blk", None), P("rep", "blk", None), P("rep", "blk", None)),
        out_specs=(P("blk", None), P("blk")),
        check_vma=False,
    )
```

```python
import functools
import math

import jax
import jax.numpy as jnp
from jax import lax
from jax.experimental import pallas as pl
from jax.experimental.pallas import tpu as pltpu
from jax.sharding import PartitionSpec as P

MESH = pl.DeviceIdType.MESH
SHARPNESS = 2.5
PARTS = 2
CHUNKS = 4
TO_NEXT_CHIP, TO_NEXT, TO_CORE, SIDE, SIDE_L, BACK, BACK_L, OWN, OWN_L, HOME, HOME_L, HOME2, HOME2_L, FINAL = range(14)
NEVER = -1e30
RING = 8


def as_column(tile, rows):
    return jnp.broadcast_to(tile[0:1], (128, rows)).T[:, 0:1]


def as_tile(column, rows):
    return jnp.broadcast_to(column, (rows, 128)).T[0:8]


def log_sum(terms):
    top = functools.reduce(jnp.maximum, terms)
    return top + jnp.log(sum(jnp.exp(t - top) for t in terms))


def kernel(
    n, q_hbm, k_hbm, v_hbm, out_hbm, log_ref,
    qs, ks, kt, vs, pf, r1, p3, r3, xs, rx, ms, rm, own, fin, lp, l1, l3, lo, lx, lm, lr,
    load_sem, send_sem, recv_sem, out_sem, ready,
):
    b = lax.axis_index("blk")
    r = lax.axis_index("rep")
    c = lax.rem(b, 2)
    place = lax.rem(b // 2, RING)
    block, depth = q_hbm.shape
    half = vs.shape[1] // 2
    rows = block // PARTS
    few = block // CHUNKS
    each = CHUNKS // PARTS

    def at(step, rep=None):
        return (lax.rem(b + n + step, n), r if rep is None else rep)

    partner = at(1 - 2 * c)

    def part(g):
        return pl.ds(g * rows, rows)

    def chunk(i):
        return pl.ds(i * few, few)

    def remote(kind, g, src, dst, device, land=None):
        return pltpu.make_async_remote_copy(
            src_ref=src, dst_ref=dst,
            send_sem=send_sem.at[kind, g],
            recv_sem=recv_sem.at[kind if land is None else land, g],
            device_id=device, device_id_type=MESH,
        )

    loads = [pltpu.make_async_copy(q_hbm, qs.at[0], load_sem.at[0]),
             pltpu.make_async_copy(k_hbm.at[0], ks, load_sem.at[1]),
             pltpu.make_async_copy(v_hbm.at[0], vs, load_sem.at[2])]
    for load in loads:
        load.start()

    barrier = pltpu.get_barrier_semaphore()
    for device in (at(-2), at(-2, 1 - r), at(-1), at(0, 1 - r)):
        pl.semaphore_signal(barrier, inc=1, device_id=device, device_id_type=MESH)

    @pl.when(c == 0)
    def _():
        pl.semaphore_signal(barrier, inc=1, device_id=partner, device_id_type=MESH)

    loads[0].wait()
    pl.semaphore_wait(barrier, 4 + c)
    pl.semaphore_signal(ready.at[0], inc=1, device_id=at(1), device_id_type=MESH)
    for rep in range(2):
        pl.semaphore_signal(ready.at[1], inc=1, device_id=at(2, rep), device_id_type=MESH)

    def next_chip(i):
        return remote(TO_NEXT_CHIP, i, qs.at[0, chunk(i)], qs.at[2, chunk(i)], at(2))

    def next_block(i):
        return remote(TO_NEXT, i, qs.at[2, chunk(i)], qs.at[3, chunk(i)], at(1))

    def next_core(i):
        return remote(TO_CORE, i, qs.at[2 * c, chunk(i)], qs.at[1, chunk(i)], partner)

    def side(g):
        return (remote(SIDE, g, pf.at[1, :, part(g)], r1.at[:, part(g)], partner),
                remote(SIDE_L, g, lp.at[1, g], l1.at[g], partner))

    def back(g):
        return (remote(BACK, g, p3.at[:, part(g)], r3.at[:, part(g)], at(-1)),
                remote(BACK_L, g, lp.at[3, g], l3.at[g], at(-1)))

    def across(g):
        return (remote(OWN, g, xs.at[part(g)], rx.at[part(g)], at(0, 1 - r)),
                remote(OWN_L, g, lo.at[g], lx.at[g], at(0, 1 - r)))

    def home(g, j, source):
        return (remote(HOME + 2 * j, g, ms.at[j, part(g)], rm.at[source, part(g)], at(-2, j), HOME + 2 * source),
                remote(HOME_L + 2 * j, g, lm.at[g], lr.at[source, g], at(-2, j), HOME_L + 2 * source))

    def final(g, column):
        return remote(FINAL, g, fin.at[part(g)], out_hbm.at[part(g), column], at(0, 1 - r))

    def start(*copies):
        for copy in copies:
            copy.start()

    def arrived(*copies):
        for copy in copies:
            copy.wait_recv()

    scale = SHARPNESS / math.sqrt(depth)

    def attend(slot, g):
        d = jnp.dot(qs[slot, part(g)], kt[...], preferred_element_type=jnp.float32)
        top = jnp.max(d, axis=1, keepdims=True)
        weights = jnp.exp2((d - top) * (scale * math.log2(math.e)))
        total = jnp.sum(weights, axis=1, keepdims=True)
        low = weights.astype(jnp.bfloat16)
        share = 1.0 / total
        for j in range(2):
            pf[slot, j, part(g)] = share * jnp.dot(low, vs[:, j * half:(j + 1) * half], preferred_element_type=jnp.float32)
        lp[slot, g] = as_tile(top * scale + jnp.log(total), rows)

    def chunks_of(g):
        return range(g * each, (g + 1) * each)

    @pl.when(c == 0)
    def _():
        for i in range(CHUNKS):
            next_core(i).start()

    @pl.when(c == 1)
    def _():
        for i in range(CHUNKS):
            next_chip(i).start()

    @pl.when(jnp.logical_and(c == 0, place == 0))
    def _():
        for i in range(CHUNKS):
            next_chip(i).start()

    loads[1].wait()

    @pl.loop(0, ks.shape[0] // 256)
    def _(i):
        columns = pl.ds(pl.multiple_of(i * 256, 256), 256)
        kt[:, columns] = ks[columns, :].T

    loads[2].wait()
    for g in range(PARTS):
        attend(0, g)

    for g in range(PARTS):
        @pl.when(c == 1)
        def _():
            for i in chunks_of(g):
                arrived(next_chip(i))
                start(next_block(i), next_core(i))
        for i in chunks_of(g):
            arrived(next_core(i))
        attend(1, g)
        start(*side(g))

        @pl.when(jnp.logical_and(c == 0, place == 1))
        def _():
            for i in chunks_of(g):
                next_chip(i).start()

    def returned(g):
        p3[:, part(g)] = pf[3, :, part(g)].astype(jnp.bfloat16)
        if g == 0:
            pl.semaphore_wait(ready.at[0], 1)
        start(*back(g))

    for g in range(PARTS):
        @pl.when(c == 0)
        def _():
            for i in chunks_of(g):
                arrived(next_block(i))

        @pl.when(jnp.logical_and(c == 0, place >= 2))
        def _():
            for i in chunks_of(g):
                next_chip(i).start()
        attend(3 - c, g)

        @pl.when(c == 0)
        def _():
            returned(g)

    for g in range(PARTS):
        arrived(*side(g))
        ours = as_column(lp[0, g], rows)
        theirs = jnp.where(c == 0, as_column(l1[g], rows), NEVER)
        both = log_sum([ours, theirs])
        ours, theirs = jnp.exp(ours - both), jnp.exp(theirs - both)
        xs[part(g)] = (ours * pf[0, 1 - r, part(g)] + theirs * r1[1 - r, part(g)]).astype(jnp.bfloat16)
        own[part(g)] = ours * pf[0, r, part(g)] + theirs * r1[r, part(g)]
        lo[g] = as_tile(both, rows)
        start(*across(g))

    def merge(g):
        if g == 0:
            pl.semaphore_wait(ready.at[1], 2)
        arrived(*back(g))
        mine = as_column(lp[2, g], rows)
        core = jnp.where(c == 1, as_column(l1[g], rows), NEVER)
        behind = as_column(l3[g], rows)
        both = log_sum([mine, core, behind])
        mine, core, behind = jnp.exp(mine - both), jnp.exp(core - both), jnp.exp(behind - both)
        lm[g] = as_tile(both, rows)
        for j in range(2):
            ms[j, part(g)] = (mine * pf[2, j, part(g)] + core * r1[j, part(g)]
                              + behind * r3[j, part(g)].astype(jnp.float32)).astype(jnp.bfloat16)
            start(*home(g, j, r))

    for g in range(PARTS):
        @pl.when(c == 0)
        def _():
            for i in chunks_of(g):
                arrived(next_chip(i))
                start(next_block(i))

        @pl.when(c == 1)
        def _():
            merge(g)
            for i in chunks_of(g):
                arrived(next_block(i))
        attend(2 + c, g)

        @pl.when(c == 1)
        def _():
            returned(g)

        @pl.when(c == 0)
        def _():
            merge(g)

    column = pl.ds(pl.multiple_of(r * half, half), half)
    outs = []
    for g in range(PARTS):
        arrived(*across(g), *home(g, 0, 0), *home(g, 1, 1))
        logs = [as_column(t, rows) for t in (lo[g], lx[g], lr[0, g], lr[1, g])]
        both = log_sum(logs)
        w = [jnp.exp(t - both) for t in logs]
        fin[part(g)] = (w[0] * own[part(g)] + w[1] * rx[part(g)].astype(jnp.float32)
                        + w[2] * rm[0, part(g)].astype(jnp.float32)
                        + w[3] * rm[1, part(g)].astype(jnp.float32)).astype(jnp.bfloat16)
        final(g, column).start()
        out = pltpu.make_async_copy(fin.at[part(g)], out_hbm.at[part(g), column], out_sem.at[g])
        out.start()
        outs.append(out)
        log_ref[g:g + 1] = as_tile(both, rows)[0:1]

    for out in outs:
        out.wait()
    for g in range(PARTS):
        arrived(final(g, column))
        for copy in (*side(g), *back(g), *across(g),
                     *home(g, 0, r), *home(g, 1, r), final(g, column)):
            copy.wait_send()
    for i in range(CHUNKS):
        for copy in (next_chip(i), next_block(i), next_core(i)):
            copy.wait_send()


def settle(attributed, log_total, out, log_out):
    out[...] = attributed[...]
    rows = log_total.shape[1]
    for g in range(log_total.shape[0]):
        log_out[pl.ds(g * rows, rows)] = log_total[g]


def shards(n, queries, corpus, attributions):
    block, depth = queries.shape
    slab, width = attributions.shape[1:]
    rows, half = block // PARTS, width // 2
    low, full = jnp.bfloat16, jnp.float32
    hbm = pl.BlockSpec(memory_space=pl.ANY)
    attributed, log_total = pl.pallas_call(
        functools.partial(kernel, n),
        out_shape=(jax.ShapeDtypeStruct((block, width), low), jax.ShapeDtypeStruct((PARTS, rows), full)),
        in_specs=[hbm] * 3,
        out_specs=(hbm, pl.BlockSpec(memory_space=pltpu.VMEM)),
        scratch_shapes=[
            pltpu.VMEM((4, block, depth), low),
            pltpu.VMEM((slab, depth), low),
            pltpu.VMEM((depth, slab), low),
            pltpu.VMEM((slab, width), low),
            pltpu.VMEM((4, 2, block, half), full),
            pltpu.VMEM((2, block, half), full),
            pltpu.VMEM((2, block, half), low),
            pltpu.VMEM((2, block, half), low),
            pltpu.VMEM((block, half), low),
            pltpu.VMEM((block, half), low),
            pltpu.VMEM((2, block, half), low),
            pltpu.VMEM((2, block, half), low),
            pltpu.VMEM((block, half), full),
            pltpu.VMEM((block, half), low),
            pltpu.VMEM((4, PARTS, 8, rows), full),
            pltpu.VMEM((PARTS, 8, rows), full),
            pltpu.VMEM((PARTS, 8, rows), full),
            pltpu.VMEM((PARTS, 8, rows), full),
            pltpu.VMEM((PARTS, 8, rows), full),
            pltpu.VMEM((PARTS, 8, rows), full),
            pltpu.VMEM((2, PARTS, 8, rows), full),
            pltpu.SemaphoreType.DMA((3,)),
            pltpu.SemaphoreType.DMA((14, CHUNKS)),
            pltpu.SemaphoreType.DMA((14, CHUNKS)),
            pltpu.SemaphoreType.DMA((PARTS,)),
            pltpu.SemaphoreType.REGULAR((2,)),
        ],
        compiler_params=pltpu.CompilerParams(collective_id=0, has_side_effects=True, vmem_limit_bytes=60 << 20),
    )(queries, corpus, attributions)
    return pl.pallas_call(
        settle,
        out_shape=(jax.ShapeDtypeStruct((block, width), low), jax.ShapeDtypeStruct((block,), full)),
        in_specs=[pl.BlockSpec(memory_space=pltpu.VMEM)] * 2,
        out_specs=(pl.BlockSpec(memory_space=pltpu.VMEM), pl.BlockSpec(memory_space=pltpu.VMEM)),
    )(attributed, log_total)


def solution(mesh):
    return jax.shard_map(
        functools.partial(shards, mesh.shape["blk"]),
        mesh=mesh,
        in_specs=(P("blk", None), P("rep", "blk", None), P("rep", "blk", None)),
        out_specs=(P("blk", None), P("blk")),
        check_vma=False,
    )
```

```python
import functools
import math

import jax
import jax.numpy as jnp
from jax import lax
from jax.experimental import pallas as pl
from jax.experimental.pallas import tpu as pltpu
from jax.sharding import PartitionSpec as P

MESH = pl.DeviceIdType.MESH
SHARPNESS = 2.5
PARTS = 2
CHUNKS = 4
TO_NEXT_CHIP, TO_NEXT, TO_CORE, SIDE, SIDE_L, BACK, BACK_L, OWN, OWN_L, HOME, HOME_L, HOME2, HOME2_L, FINAL = range(14)
NEVER = -1e30
RING = 8


def as_column(tile, rows):
    return jnp.broadcast_to(tile[0:1], (128, rows)).T[:, 0:1]


def as_tile(column, rows):
    return jnp.broadcast_to(column, (rows, 128)).T[0:8]


def log_sum(terms):
    top = functools.reduce(jnp.maximum, terms)
    return top + jnp.log(sum(jnp.exp(t - top) for t in terms))


def kernel(
    n, q_hbm, k_hbm, v_hbm, out_hbm, log_ref,
    qs, ks, kt, vs, pf, r1, p3, r3, xs, rx, ms, rm, own, fin, lp, l1, l3, lo, lx, lm, lr,
    load_sem, send_sem, recv_sem, out_sem, ready,
):
    b = lax.axis_index("blk")
    r = lax.axis_index("rep")
    c = lax.rem(b, 2)
    place = lax.rem(b // 2, RING)
    block, depth = q_hbm.shape
    half = vs.shape[1] // 2
    rows = block // PARTS
    few = block // CHUNKS
    each = CHUNKS // PARTS

    def at(step, rep=None):
        return (lax.rem(b + n + step, n), r if rep is None else rep)

    partner = at(1 - 2 * c)

    def part(g):
        return pl.ds(g * rows, rows)

    def chunk(i):
        return pl.ds(i * few, few)

    def remote(kind, g, src, dst, device, land=None):
        return pltpu.make_async_remote_copy(
            src_ref=src, dst_ref=dst,
            send_sem=send_sem.at[kind, g],
            recv_sem=recv_sem.at[kind if land is None else land, g],
            device_id=device, device_id_type=MESH,
        )

    loads = [pltpu.make_async_copy(q_hbm, qs.at[0], load_sem.at[0]),
             pltpu.make_async_copy(k_hbm.at[0], ks, load_sem.at[1]),
             pltpu.make_async_copy(v_hbm.at[0], vs, load_sem.at[2])]
    for load in loads:
        load.start()

    barrier = pltpu.get_barrier_semaphore()
    for device in (at(-2), at(-2, 1 - r), at(-1), at(0, 1 - r)):
        pl.semaphore_signal(barrier, inc=1, device_id=device, device_id_type=MESH)

    @pl.when(c == 0)
    def _():
        pl.semaphore_signal(barrier, inc=1, device_id=partner, device_id_type=MESH)

    loads[0].wait()
    pl.semaphore_wait(barrier, 4 + c)
    pl.semaphore_signal(ready.at[0], inc=1, device_id=at(1), device_id_type=MESH)
    for rep in range(2):
        pl.semaphore_signal(ready.at[1], inc=1, device_id=at(2, rep), device_id_type=MESH)

    def next_chip(i):
        return remote(TO_NEXT_CHIP, i, qs.at[0, chunk(i)], qs.at[2, chunk(i)], at(2))

    def next_block(i):
        return remote(TO_NEXT, i, qs.at[2, chunk(i)], qs.at[3, chunk(i)], at(1))

    def next_core(i):
        return remote(TO_CORE, i, qs.at[2 * c, chunk(i)], qs.at[1, chunk(i)], partner)

    def side(g):
        return (remote(SIDE, g, pf.at[1, :, part(g)], r1.at[:, part(g)], partner),
                remote(SIDE_L, g, lp.at[1, g], l1.at[g], partner))

    def back(g):
        return (remote(BACK, g, p3.at[:, part(g)], r3.at[:, part(g)], at(-1)),
                remote(BACK_L, g, lp.at[3, g], l3.at[g], at(-1)))

    def across(g):
        return (remote(OWN, g, xs.at[part(g)], rx.at[part(g)], at(0, 1 - r)),
                remote(OWN_L, g, lo.at[g], lx.at[g], at(0, 1 - r)))

    def home(i, j, source):
        return remote(HOME + 2 * j, i, ms.at[j, chunk(i)], rm.at[source, chunk(i)], at(-2, j), HOME + 2 * source)

    def home_l(g, j, source):
        return remote(HOME_L + 2 * j, g, lm.at[g], lr.at[source, g], at(-2, j), HOME_L + 2 * source)

    def final(i, column):
        return remote(FINAL, i, fin.at[chunk(i)], out_hbm.at[chunk(i), column], at(0, 1 - r))

    def start(*copies):
        for copy in copies:
            copy.start()

    def arrived(*copies):
        for copy in copies:
            copy.wait_recv()

    scale = SHARPNESS / math.sqrt(depth)

    def attend(slot, g):
        d = jnp.dot(qs[slot, part(g)], kt[...], preferred_element_type=jnp.float32)
        top = jnp.max(d, axis=1, keepdims=True)
        weights = jnp.exp2((d - top) * (scale * math.log2(math.e)))
        total = jnp.sum(weights, axis=1, keepdims=True)
        low = weights.astype(jnp.bfloat16)
        share = 1.0 / total
        for j in range(2):
            pf[slot, j, part(g)] = share * jnp.dot(low, vs[:, j * half:(j + 1) * half], preferred_element_type=jnp.float32)
        lp[slot, g] = as_tile(top * scale + jnp.log(total), rows)

    def chunks_of(g):
        return range(g * each, (g + 1) * each)

    @pl.when(c == 0)
    def _():
        for i in range(CHUNKS):
            next_core(i).start()

    @pl.when(c == 1)
    def _():
        for i in range(CHUNKS):
            next_chip(i).start()

    loads[1].wait()

    @pl.loop(0, ks.shape[0] // 256)
    def _(i):
        columns = pl.ds(pl.multiple_of(i * 256, 256), 256)
        kt[:, columns] = ks[columns, :].T

    loads[2].wait()
    for g in range(PARTS):
        attend(0, g)

    @pl.when(jnp.logical_and(c == 0, place == 0))
    def _():
        for i in range(CHUNKS):
            next_chip(i).start()

    for g in range(PARTS):
        @pl.when(c == 1)
        def _():
            for i in chunks_of(g):
                arrived(next_chip(i))
                start(next_block(i), next_core(i))
        for i in chunks_of(g):
            arrived(next_core(i))
        attend(1, g)
        start(*side(g))

        @pl.when(jnp.logical_and(c == 0, place == 1))
        def _():
            for i in chunks_of(g):
                next_chip(i).start()

    def returned(g):
        p3[:, part(g)] = pf[3, :, part(g)].astype(jnp.bfloat16)
        if g == 0:
            pl.semaphore_wait(ready.at[0], 1)
        start(*back(g))

    for g in range(PARTS):
        @pl.when(c == 0)
        def _():
            for i in chunks_of(g):
                arrived(next_block(i))

        @pl.when(jnp.logical_and(c == 0, place >= 2))
        def _():
            for i in chunks_of(g):
                next_chip(i).start()
        attend(3 - c, g)

        @pl.when(c == 0)
        def _():
            returned(g)

    for g in range(PARTS):
        arrived(*side(g))
        ours = as_column(lp[0, g], rows)
        theirs = jnp.where(c == 0, as_column(l1[g], rows), NEVER)
        both = log_sum([ours, theirs])
        ours, theirs = jnp.exp(ours - both), jnp.exp(theirs - both)
        xs[part(g)] = (ours * pf[0, 1 - r, part(g)] + theirs * r1[1 - r, part(g)]).astype(jnp.bfloat16)
        own[part(g)] = ours * pf[0, r, part(g)] + theirs * r1[r, part(g)]
        lo[g] = as_tile(both, rows)
        start(*across(g))

    def merge(g):
        if g == 0:
            pl.semaphore_wait(ready.at[1], 2)
        arrived(*back(g))
        mine = as_column(lp[2, g], rows)
        core = jnp.where(c == 1, as_column(l1[g], rows), NEVER)
        behind = as_column(l3[g], rows)
        both = log_sum([mine, core, behind])
        mine, core, behind = jnp.exp(mine - both), jnp.exp(core - both), jnp.exp(behind - both)
        lm[g] = as_tile(both, rows)
        for j in (1 - r, r):
            start(home_l(g, j, r))
        for i in chunks_of(g):
            these = slice((i - g * each) * few, (i - g * each + 1) * few)
            for j in (1 - r, r):
                ms[j, chunk(i)] = (mine[these] * pf[2, j, chunk(i)] + core[these] * r1[j, chunk(i)]
                                   + behind[these] * r3[j, chunk(i)].astype(jnp.float32)).astype(jnp.bfloat16)
                start(home(i, j, r))

    for g in range(PARTS):
        @pl.when(c == 0)
        def _():
            for i in chunks_of(g):
                arrived(next_chip(i))
                start(next_block(i))

        @pl.when(c == 1)
        def _():
            merge(g)
            for i in chunks_of(g):
                arrived(next_block(i))
        attend(2 + c, g)

        @pl.when(c == 1)
        def _():
            returned(g)

        @pl.when(c == 0)
        def _():
            merge(g)

    column = pl.ds(pl.multiple_of(r * half, half), half)
    outs = []
    for g in range(PARTS):
        arrived(*across(g), home_l(g, 0, 0), home_l(g, 1, 1))
        logs = [as_column(t, rows) for t in (lo[g], lx[g], lr[0, g], lr[1, g])]
        both = log_sum(logs)
        w = [jnp.exp(t - both) for t in logs]
        log_ref[g:g + 1] = as_tile(both, rows)[0:1]
        for i in chunks_of(g):
            these = slice((i - g * each) * few, (i - g * each + 1) * few)
            arrived(home(i, 0, 0), home(i, 1, 1))
            fin[chunk(i)] = (w[0][these] * own[chunk(i)] + w[1][these] * rx[chunk(i)].astype(jnp.float32)
                             + w[2][these] * rm[0, chunk(i)].astype(jnp.float32)
                             + w[3][these] * rm[1, chunk(i)].astype(jnp.float32)).astype(jnp.bfloat16)
            final(i, column).start()
            out = pltpu.make_async_copy(fin.at[chunk(i)], out_hbm.at[chunk(i), column], out_sem.at[i])
            out.start()
            outs.append(out)

    for out in outs:
        out.wait()
    for g in range(PARTS):
        for copy in (*side(g), *back(g), *across(g), home_l(g, 0, r), home_l(g, 1, r)):
            copy.wait_send()
    for i in range(CHUNKS):
        arrived(final(i, column))
        for copy in (home(i, 0, r), home(i, 1, r), final(i, column)):
            copy.wait_send()
    for i in range(CHUNKS):
        for copy in (next_chip(i), next_block(i), next_core(i)):
            copy.wait_send()


def settle(attributed, log_total, out, log_out):
    out[...] = attributed[...]
    rows = log_total.shape[1]
    for g in range(log_total.shape[0]):
        log_out[pl.ds(g * rows, rows)] = log_total[g]


def shards(n, queries, corpus, attributions):
    block, depth = queries.shape
    slab, width = attributions.shape[1:]
    rows, half = block // PARTS, width // 2
    low, full = jnp.bfloat16, jnp.float32
    hbm = pl.BlockSpec(memory_space=pl.ANY)
    attributed, log_total = pl.pallas_call(
        functools.partial(kernel, n),
        out_shape=(jax.ShapeDtypeStruct((block, width), low), jax.ShapeDtypeStruct((PARTS, rows), full)),
        in_specs=[hbm] * 3,
        out_specs=(hbm, pl.BlockSpec(memory_space=pltpu.VMEM)),
        scratch_shapes=[
            pltpu.VMEM((4, block, depth), low),
            pltpu.VMEM((slab, depth), low),
            pltpu.VMEM((depth, slab), low),
            pltpu.VMEM((slab, width), low),
            pltpu.VMEM((4, 2, block, half), full),
            pltpu.VMEM((2, block, half), full),
            pltpu.VMEM((2, block, half), low),
            pltpu.VMEM((2, block, half), low),
            pltpu.VMEM((block, half), low),
            pltpu.VMEM((block, half), low),
            pltpu.VMEM((2, block, half), low),
            pltpu.VMEM((2, block, half), low),
            pltpu.VMEM((block, half), full),
            pltpu.VMEM((block, half), low),
            pltpu.VMEM((4, PARTS, 8, rows), full),
            pltpu.VMEM((PARTS, 8, rows), full),
            pltpu.VMEM((PARTS, 8, rows), full),
            pltpu.VMEM((PARTS, 8, rows), full),
            pltpu.VMEM((PARTS, 8, rows), full),
            pltpu.VMEM((PARTS, 8, rows), full),
            pltpu.VMEM((2, PARTS, 8, rows), full),
            pltpu.SemaphoreType.DMA((3,)),
            pltpu.SemaphoreType.DMA((14, CHUNKS)),
            pltpu.SemaphoreType.DMA((14, CHUNKS)),
            pltpu.SemaphoreType.DMA((CHUNKS,)),
            pltpu.SemaphoreType.REGULAR((2,)),
        ],
        compiler_params=pltpu.CompilerParams(collective_id=0, has_side_effects=True, vmem_limit_bytes=60 << 20),
    )(queries, corpus, attributions)
    return pl.pallas_call(
        settle,
        out_shape=(jax.ShapeDtypeStruct((block, width), low), jax.ShapeDtypeStruct((block,), full)),
        in_specs=[pl.BlockSpec(memory_space=pltpu.VMEM)] * 2,
        out_specs=(pl.BlockSpec(memory_space=pltpu.VMEM), pl.BlockSpec(memory_space=pltpu.VMEM)),
    )(attributed, log_total)


def solution(mesh):
    return jax.shard_map(
        functools.partial(shards, mesh.shape["blk"]),
        mesh=mesh,
        in_specs=(P("blk", None), P("rep", "blk", None), P("rep", "blk", None)),
        out_specs=(P("blk", None), P("blk")),
        check_vma=False,
    )
```
